128 devices in a mesh: ep: 8 (over x_lo, y), tp: 16 (over x_hi, z, core).
Axes of the slice: x: 4 (x_hi: 2, x_lo: 2; x = x_hi * 2 + x_lo), y: 4, z: 4, core: 2. Of those that a mesh axis runs over, the one named last changes fastest.
Arguments:
- tokens: bfloat16 [1024, 6144], P('ep'), may hold values from -6 to 6
- expert_ids: int32 [1024, 2], P('ep'), may hold values from 0 to 7, all different within a row; in each aligned block of 128 rows (0 to 127, 128 to 255, ...) at most 48 rows name the same one
- router: bfloat16 [6144, 8], replicated, may hold values from -0.078125 to 0.078125
- gate_weight: bfloat16 [8, 6144, 8192], P('ep', None, 'tp'), may hold values from -0.078125 to 0.078125
- up_weight: bfloat16 [8, 6144, 8192], P('ep', None, 'tp'), may hold values from -0.078125 to 0.078125
- down_weight: bfloat16 [8, 8192, 6144], P('ep', 'tp'), may hold values from -0.0625 to 0.0625
- keep_mask: int32 [1024, 6144], P('ep'), may hold values 0 or 1
Outputs:
- layer_out: bfloat16 [1024, 6144], P('ep')
The draws below stay inside these ranges and needn't reach their ends.
Inputs may be any that keep to these rules, and one draw needn't show every extreme that they name: `expert_ids`: each row names two different experts. In the rows of one token block of 128 rows no expert is named more than 48 times, a bound that some block reaches.
All inputs are finite; a program needn't handle non-finite values. No bound on the sum of `keep_mask` on one device may be relied on, other than what follows from the above.
Results may differ from the reference program's by a relative error of at most 0.018.
Values may be sent and summed in bfloat16 or wider, within the bound.
A program may use at most 128 MiB of HBM per device.

```python
import math
import jax
import jax.numpy as jnp
import numpy as np
from jax import lax

D = 6144
FF = 8192
TOK_DEV = 128
EXPERTS = 8
CAP = 48
TOKENS = 1024
N_EP = 8
N_TP = 16


def set_ends(drawn, rng, smallest, top_value):
    index_at = [jax.random.randint(jax.random.fold_in(rng, axis), (), 0, length) for axis, length in enumerate(drawn.shape)]
    longest = drawn.shape.index(max(drawn.shape))
    next_to = index_at[:longest] + [(index_at[longest] + 1) % drawn.shape[longest]] + index_at[longest + 1:]
    return drawn.at[tuple(index_at)].set(smallest).at[tuple(next_to)].set(top_value)


def levels(key, extent, pieces, least, largest):
    def one(dim, shards_of):
        steps = jax.random.uniform(jax.random.fold_in(jax.random.fold_in(key, 6), dim), (shards_of,), jnp.float32, least / len(pieces), largest / len(pieces))
        return jnp.repeat(jnp.exp(steps), extent[dim] // shards_of).reshape((-1,) + (1,) * (len(extent) - dim - 1))

    gain = one(*pieces[0])
    for cut in pieces[1:]:
        gain = gain * one(*cut)
    return gain


def assign_block(key, own, number, rows, count, top, limit, skew):
    ranking = jax.random.permutation(key, count)
    heavy_load, ordinary = shares(count, rows * top, limit, skew, True), shares(count, rows * top, limit, skew, False)
    places = jnp.arange(count)

    def named(tallies, offset_by):
        used = int((tallies > 0).sum())
        fixed = max(1, used // 4)
        moved = fixed + (places - fixed + offset_by * (used - fixed)) % max(1, count - fixed)
        return jnp.zeros((count,), jnp.int32).at[ranking[jnp.where(places < fixed, places, moved)]].set(jnp.asarray(tallies, jnp.int32))

    tallies = jnp.where(number % 4 == 0, named(heavy_load, number // 4), named(ordinary, number - number // 4 - 1))
    mixed = jax.random.permutation(jax.random.fold_in(own, 3), count)
    source_of, receiver = mixed[0:count // 2 * 2:2], mixed[1:count // 2 * 2:2]
    slack = jnp.minimum(tallies[source_of] - 1, limit - tallies[receiver]) // 2
    slack = jnp.where((source_of == ranking[0]) | (receiver == ranking[0]) | (tallies[receiver] == 0), 0, jnp.maximum(slack, 0))
    moved = jax.random.randint(jax.random.fold_in(own, 4), (count // 2,), 0, 1 << 20) % (slack + 1)
    tallies = tallies.at[source_of].add(-moved).at[receiver].add(moved)
    labels = jnp.searchsorted(jnp.cumsum(tallies), jnp.arange(rows * top), side="right").astype(jnp.int32)
    listing = labels.reshape(top, rows).T
    listing = listing[jax.random.permutation(jax.random.fold_in(own, 1), rows)]
    offset_by = jax.random.randint(jax.random.fold_in(own, 2), (rows, 1), 0, top)
    return jnp.take_along_axis(listing, (jnp.arange(top)[None, :] + offset_by) % top, axis=1)


def shares(count, total, bound, slope, full):
    weights = [(1 << 20) // math.isqrt(rank ** slope) + 1 for rank in range(1, count + 1)]
    largest = bound if full else min(bound, max(-(-total // count), total * weights[0] // sum(weights)))
    least = 1 if total - largest >= count - 1 else 0
    holding, rest = [largest] + [least] * (count - 1), total - largest - least * (count - 1)
    while rest > 0:
        movable = [i for i in range(1, count) if holding[i] < largest] or [i for i in range(1, count) if holding[i] < bound]
        mass, budget = sum([weights[i] for i in movable]), rest
        for i in movable:
            more = min(bound - holding[i], max(1, budget * weights[i] // mass), rest)
            holding[i] = holding[i] + more
            rest = rest - more
    return np.array(holding)


def centred(own_key, extent, spread, limit, split=(), kind=jnp.bfloat16):
    values = jax.random.normal(own_key, extent, jnp.float32) * spread
    if len(split) > 0:
        values = levels(own_key, extent, split, -0.22, 0.18) * values
    return jnp.clip(values, min=-limit, max=limit).astype(kind)


def setup_inputs(seed: int = 0) -> dict:
    splits = jax.random.split(jax.random.key(seed), 8)
    tokens = centred(splits[0], (TOKENS, D), 1.0, 6.0, ((0, 8),))
    expert_ids_keys = jax.random.split(jax.random.fold_in(splits[1], 1), TOKENS // TOK_DEV)
    expert_ids_turns = jax.random.permutation(jax.random.fold_in(splits[1], 3), TOKENS // TOK_DEV)
    expert_ids = jax.vmap(lambda own, number: assign_block(jax.random.fold_in(splits[1], 2), own, number, TOK_DEV, EXPERTS, 2, CAP, 2))(expert_ids_keys, expert_ids_turns).reshape((TOKENS, 2))
    router = centred(splits[2], (D, EXPERTS), D ** -0.5, 0.078125)
    gate_weight = centred(splits[3], (EXPERTS, D, FF), D ** -0.5, 0.078125, ((0, 8), (2, 16)))
    up_weight = centred(splits[4], (EXPERTS, D, FF), D ** -0.5, 0.078125, ((0, 8), (2, 16)))
    down_weight = centred(splits[5], (EXPERTS, FF, D), FF ** -0.5, 0.0625, ((0, 8), (1, 16)))
    keep_mask = set_ends((jax.random.randint(splits[6], (TOKENS, D), 0, 5) < 4).astype(jnp.int32), jax.random.fold_in(splits[6], 1), 0, 1)
    return dict(tokens=tokens, expert_ids=expert_ids, router=router, gate_weight=gate_weight, up_weight=up_weight, down_weight=down_weight, keep_mask=keep_mask)


def reference(tokens, expert_ids, router, gate_weight, up_weight, down_weight, keep_mask):
    total_rows = tokens.shape[0]
    logits = jnp.dot(tokens, router, preferred_element_type=jnp.float32)
    picked = jnp.take_along_axis(logits, expert_ids, axis=1)
    weight_first = jax.nn.sigmoid(picked[:, 0] - picked[:, 1])
    weight_second = jax.nn.sigmoid(picked[:, 1] - picked[:, 0])
    onehot = (expert_ids[:, :, None] == jnp.arange(EXPERTS, dtype=jnp.int32)[None, None, :]).astype(jnp.int32)
    blocked = onehot.reshape(N_EP, TOK_DEV * 2, EXPERTS)
    ranks = jnp.cumsum(blocked, axis=1) - blocked
    slot = jnp.sum(ranks * blocked, axis=2).reshape(total_rows, 2)
    block_of = jnp.arange(total_rows, dtype=jnp.int32) // TOK_DEV
    place = (block_of[:, None] * CAP + slot).astype(jnp.int32)
    token_index = jnp.broadcast_to(jnp.arange(total_rows, dtype=jnp.int32)[:, None], (total_rows, 2))
    table = jnp.full((EXPERTS, N_EP * CAP), total_rows, jnp.int32)
    table = table.at[expert_ids, place].set(token_index)
    padded = jnp.concatenate([tokens, jnp.zeros((1, tokens.shape[1]), jnp.bfloat16)], axis=0)
    width = FF // N_TP

    def one_expert(inputs):
        w_gate, w_up, w_down, rows_index = inputs
        buffer = jnp.take(padded, rows_index, axis=0)
        gate = jnp.dot(buffer, w_gate, preferred_element_type=jnp.float32)
        up = jnp.dot(buffer, w_up, preferred_element_type=jnp.float32)
        hidden = (jax.nn.silu(gate) * up).astype(jnp.bfloat16)

        def add_block(block, total):
            start = (block * width).astype(jnp.int32)
            h_block = lax.dynamic_slice_in_dim(hidden, start, width, 1)
            d_block = lax.dynamic_slice_in_dim(w_down, start, width, 0)
            partial_sum = jnp.dot(h_block, d_block, preferred_element_type=jnp.float32)
            rounded = lax.optimization_barrier(partial_sum.astype(jnp.bfloat16))
            return total + rounded.astype(jnp.float32)

        empty = jnp.zeros((buffer.shape[0], buffer.shape[1]), jnp.float32)
        summed = lax.fori_loop(0, N_TP, add_block, empty)
        return summed.astype(jnp.bfloat16)

    outputs = lax.map(one_expert, (gate_weight, up_weight, down_weight, table))
    first_rows = outputs[expert_ids[:, 0], place[:, 0]].astype(jnp.float32)
    second_rows = outputs[expert_ids[:, 1], place[:, 1]].astype(jnp.float32)
    combined = weight_first[:, None] * first_rows + weight_second[:, None] * second_rows
    return (combined * keep_mask.astype(jnp.float32) * 1.25).astype(jnp.bfloat16)
```

```python
import functools

import jax
import jax.numpy as jnp
from jax import lax
from jax.experimental import pallas as pl
from jax.experimental.pallas import tpu as pltpu
from jax.sharding import PartitionSpec as P

MESH = pl.DeviceIdType.MESH
BF16 = jnp.bfloat16
F32 = jnp.float32
N_EP, N_TP = 8, 16
N_Z = 4
GW = 512
HOPS = [(1, 2), (0, 2), (1, 1), (1, 3), (0, 1), (0, 3), (1, 0)]
Z_HOPS = [2, 1, 3]


def dot(a, b):
    return jnp.dot(a, b, preferred_element_type=F32)


def kernel(cap, ids_ref, tok_h, rt_h, wg_h, wu_h, wd_h, mk_h, out_ref,
           tok, rt, wg, wu, wd, mk, og, oq, xg, xq, gate, up, hid, sd, rd, tt, cb,
           lsem, g_s, g_r, q_s, q_r, z_s, z_r, dg_s, dg_r, dq_s, dq_r, rd_s, rd_r,
           m_s, m_r, a_s, a_r, da_s, da_r):
    ep = lax.axis_index("ep")
    tp = lax.axis_index("tp")
    xl, y = ep // 4, ep % 4
    xh, z, c = tp // 8, (tp // 2) % N_Z, tp % 2
    tok_rows, width = tok.shape
    qw = oq.shape[2]
    rows = N_EP * cap
    rw = width // 8
    hw = rw // 2

    def ep_at(a, b):
        return ((xl + a) % 2) * 4 + (y + b) % 4

    def tp_at(h, s, k):
        return ((xh + h) % 2) * 8 + ((z + s) % N_Z) * 2 + (c + k) % 2

    barrier = pltpu.get_barrier_semaphore()
    for a in range(2):
        for b in range(4):
            for h in range(2):
                for s in range(N_Z):
                    if a or b or h or s:
                        pl.semaphore_signal(barrier, inc=1, device_id=(ep_at(a, b), tp_at(h, s, 0)), device_id_type=MESH)
    pl.semaphore_signal(barrier, inc=1, device_id=(ep, tp_at(0, 0, 1)), device_id_type=MESH)

    piece = z * 2 + c
    out_col = pl.multiple_of(piece * rw + xh * hw, 128)
    loads = [
        pltpu.make_async_copy(tok_h, tok, lsem.at[0]),
        pltpu.make_async_copy(wg_h.at[0], wg, lsem.at[1]),
        pltpu.make_async_copy(wu_h.at[0], wu, lsem.at[2]),
        pltpu.make_async_copy(wd_h.at[0], wd, lsem.at[3]),
        pltpu.make_async_copy(rt_h, rt, lsem.at[4]),
        pltpu.make_async_copy(mk_h.at[:, pl.ds(out_col, hw)], mk, lsem.at[5]),
    ]
    for cp in loads:
        cp.start()

    ids = ids_ref[...]
    id0, id1 = ids[:, 0:1], ids[:, 1:2]
    lane = lax.broadcasted_iota(jnp.int32, (tok_rows, 128), 1)
    sub = lax.broadcasted_iota(jnp.int32, (tok_rows, 128), 0)
    oh0 = (lane == id0).astype(F32)
    oh1 = (lane == id1).astype(F32)
    rlane = lax.broadcasted_iota(jnp.int32, (tok_rows, tok_rows), 1)
    rsub = lax.broadcasted_iota(jnp.int32, (tok_rows, tok_rows), 0)
    before = (rlane < rsub).astype(BF16)
    count = dot(before, (oh0 + oh1).astype(BF16))
    place0 = id0.astype(F32) * cap + jnp.sum(count * oh0, axis=1, keepdims=True)
    place1 = id1.astype(F32) * cap + jnp.sum(count * oh1, axis=1, keepdims=True)
    eye = rlane == rsub
    row0 = jnp.sum(jnp.where(eye, place0, 0.0), axis=0, keepdims=True)
    row1 = jnp.sum(jnp.where(eye, place1, 0.0), axis=0, keepdims=True)
    line = lax.broadcasted_iota(jnp.int32, (rows, tok_rows), 0).astype(F32)
    picker = ((line == row0) | (line == row1)).astype(BF16)
    loads[0].wait()
    g_col = pl.multiple_of(piece * GW, 128)
    q_col = pl.multiple_of(8 * GW + c * qw, 128)
    og[...] = dot(picker, tok[:, pl.ds(g_col, GW)]).astype(BF16).reshape(N_EP, cap, GW)
    oq[...] = dot(picker, tok[:, pl.ds(q_col, qw)]).astype(BF16).reshape(N_EP, cap, qw)
    xg[piece, ep] = og[ep]
    xq[c, ep] = oq[ep]

    pl.semaphore_wait(barrier, 64)

    def remote(src, dst, ss, rs, e, t):
        return pltpu.make_async_remote_copy(src_ref=src, dst_ref=dst, send_sem=ss, recv_sem=rs, device_id=(e, t), device_id_type=MESH)

    def arrived(dst, rs):
        remote(dst, dst, rs, rs, ep, tp_at(0, 0, 1)).wait_recv()

    def sent(src, ss):
        remote(src, src, ss, ss, ep, tp_at(0, 0, 1)).wait_send()

    twin = tp_at(0, 0, 1)
    for a, b in HOPS:
        e = ep_at(a, b)
        remote(og.at[e], xg.at[piece, ep], g_s, g_r.at[ep], e, tp).start()
    for a, b in HOPS:
        e = ep_at(a, b)
        remote(oq.at[e], xq.at[c, ep], q_s, q_r.at[ep], e, tp).start()

    def spread(d):
        for s in Z_HOPS:
            remote(xg.at[piece, d], xg.at[piece, d], z_s, z_r.at[z, d], ep, tp_at(0, s, 0)).start()
        remote(xg.at[piece, d], xg.at[piece, d], dg_s, dg_r.at[z], ep, twin).start()

    spread(ep)
    remote(xq.at[c, ep], xq.at[c, ep], dq_s, dq_r, ep, twin).start()
    order = HOPS[::-1]
    sources = [ep] + [ep_at(-a, -b + 4) for a, b in order]
    for d in sources[1:]:
        arrived(xg.at[piece, d], g_r.at[d])
        spread(d)

    gate[...] = jnp.zeros_like(gate)
    up[...] = jnp.zeros_like(up)
    loads[1].wait()
    loads[2].wait()

    def consume(x, first, size):
        k = pl.ds(pl.multiple_of(first, 128), size)
        gate[...] += dot(x, wg[k, :])
        up[...] += dot(x, wu[k, :])

    def consume_g(p):
        consume(xg[p].reshape(rows, GW), p * GW, GW)

    consume_g(piece)
    other = z * 2 + (1 - c)
    arrived(xg.at[other], dg_r.at[z])
    consume_g(other)
    for s in Z_HOPS[::-1]:
        zz = (z + s) % N_Z
        for d in sources:
            arrived(xg.at[zz * 2 + c, d], z_r.at[zz, d])
            remote(xg.at[zz * 2 + c, d], xg.at[zz * 2 + c, d], dg_s, dg_r.at[zz], ep, twin).start()
    for d in sources[1:]:
        arrived(xq.at[c, d], q_r.at[d])
        remote(xq.at[c, d], xq.at[c, d], dq_s, dq_r, ep, twin).start()
    for s in Z_HOPS[::-1]:
        zz = (z + s) % N_Z
        consume_g(zz * 2 + c)
        arrived(xg.at[zz * 2 + 1 - c], dg_r.at[zz])
        consume_g(zz * 2 + 1 - c)
    consume(xq[c].reshape(rows, qw), 8 * GW + c * qw, qw)
    arrived(xq.at[1 - c], dq_r)
    consume(xq[1 - c].reshape(rows, qw), 8 * GW + (1 - c) * qw, qw)
    hid[...] = (jax.nn.silu(gate[...]) * up[...]).astype(BF16)
    loads[3].wait()

    z_order = Z_HOPS + [0]

    def down_twin(i):
        zz = (z + z_order[i]) % N_Z
        col = pl.multiple_of((zz * 2 + 1 - c) * rw, 128)
        sd[i] = dot(hid[...], wd[:, pl.ds(col, rw)]).astype(BF16)
        remote(sd.at[i], rd.at[i], rd_s, rd_r.at[i], ep, twin).start()

    def down_own(i):
        zz = (z + z_order[i]) % N_Z
        col = pl.multiple_of((zz * 2 + c) * rw, 128)
        arrived(rd.at[i], rd_r.at[i])
        total = dot(hid[...], wd[:, pl.ds(col, rw)]) + rd[i].astype(F32)
        tt[i] = total.astype(BF16).reshape(N_EP, cap, rw)
        for h in (1, 0):
            hcol = pl.multiple_of(((xh + h) % 2) * hw, 128)
            for a, b in HOPS + [(0, 0)]:
                e = ep_at(a, b)
                src = tt.at[i, e, :, pl.ds(hcol, hw)]
                here = (xh * N_Z + z) * N_EP + ep
                if h == 0 and a == 0 and b == 0 and z_order[i] == 0:
                    cb[here] = tt[i, e, :, pl.ds(hcol, hw)]
                else:
                    remote(src, cb.at[here], m_s, m_r, e, tp_at(h, z_order[i], 0)).start()

    down_twin(0)
    down_twin(1)
    down_own(0)
    down_twin(2)
    down_own(1)
    down_twin(3)
    down_own(2)
    down_own(3)

    loads[4].wait()
    loads[5].wait()
    logits = dot(tok[...], rt[...])
    elane = lax.broadcasted_iota(jnp.int32, logits.shape, 1)
    pick0 = jnp.sum(jnp.where(elane == id0, logits, 0.0), axis=1, keepdims=True)
    pick1 = jnp.sum(jnp.where(elane == id1, logits, 0.0), axis=1, keepdims=True)
    w0 = jax.nn.sigmoid(pick0 - pick1)
    w1 = jax.nn.sigmoid(pick1 - pick0)
    keep = mk[...].astype(F32) * 1.25
    cline = lax.broadcasted_iota(jnp.int32, (tok_rows, rows), 1).astype(F32)
    sel = jnp.concatenate([(cline == place0).astype(BF16), (cline == place1).astype(BF16)], axis=0)

    n_src = cb.shape[0]
    arrived(cb.at[pl.ds(0, n_src - 1)], m_r)
    total = cb[0:N_EP].astype(F32)
    for j in range(1, n_src // N_EP):
        total += cb[j * N_EP:(j + 1) * N_EP].astype(F32)
    both = dot(sel, total.astype(BF16).reshape(rows, hw))
    combined = w0 * both[:tok_rows] + w1 * both[tok_rows:]
    mine = pl.ds(out_col, hw)
    out_ref[:, mine] = (combined * keep).astype(BF16)

    for h in (1, 0):
        for s in Z_HOPS + [0]:
            if h or s:
                remote(out_ref.at[:, mine], out_ref.at[:, mine], a_s, a_r.at[xh * N_Z + z], ep, tp_at(h, s, 0)).start()
    remote(out_ref.at[:, mine], out_ref.at[:, mine], da_s, da_r, ep, twin).start()
    for h in (0, 1):
        for s in (0, 1, 3, 2):
            if h or s:
                hh, zz = (xh + h) % 2, (z + s) % N_Z
                theirs = pl.ds(pl.multiple_of((zz * 2 + c) * rw + hh * hw, 128), hw)
                arrived(out_ref.at[:, theirs], a_r.at[hh * N_Z + zz])
                remote(out_ref.at[:, theirs], out_ref.at[:, theirs], da_s, da_r, ep, twin).start()
    arrived(out_ref.at[:, pl.ds(0, 8 * hw)], da_r)

    sent(og.at[pl.ds(0, 7)], g_s)
    sent(oq.at[pl.ds(0, 7)], q_s)
    sent(xg.at[pl.ds(0, 3)], z_s)
    sent(xg.at[pl.ds(0, 4)], dg_s)
    sent(xq.at[0], dq_s)
    sent(sd, rd_s)
    sent(cb.at[pl.ds(0, n_src - 1)], m_s)
    sent(out_ref.at[:, pl.ds(0, 7 * hw)], a_s)
    sent(out_ref.at[:, pl.ds(0, 8 * hw)], da_s)


def shards(tokens, expert_ids, router, gate_weight, up_weight, down_weight, keep_mask):
    tok_rows, width = tokens.shape
    hidden = gate_weight.shape[2]
    cap = 3 * tok_rows // N_EP
    rows = N_EP * cap
    qw = (width - 8 * GW) // 2
    rw = width // 8
    hw = rw // 2
    any_spec = pl.BlockSpec(memory_space=pl.ANY)
    vmem_spec = pl.BlockSpec(memory_space=pltpu.VMEM)
    dma = pltpu.SemaphoreType.DMA
    return pl.pallas_call(
        functools.partial(kernel, cap),
        out_shape=jax.ShapeDtypeStruct((tok_rows, width), BF16),
        in_specs=[vmem_spec] + [any_spec] * 6,
        out_specs=vmem_spec,
        scratch_shapes=[
            pltpu.VMEM((tok_rows, width), BF16),
            pltpu.VMEM(router.shape, BF16),
            pltpu.VMEM((width, hidden), BF16),
            pltpu.VMEM((width, hidden), BF16),
            pltpu.VMEM((hidden, width), BF16),
            pltpu.VMEM((tok_rows, hw), jnp.int32),
            pltpu.VMEM((N_EP, cap, GW), BF16),
            pltpu.VMEM((N_EP, cap, qw), BF16),
            pltpu.VMEM((8, N_EP, cap, GW), BF16),
            pltpu.VMEM((2, N_EP, cap, qw), BF16),
            pltpu.VMEM((rows, hidden), F32),
            pltpu.VMEM((rows, hidden), F32),
            pltpu.VMEM((rows, hidden), BF16),
            pltpu.VMEM((N_Z, rows, rw), BF16),
            pltpu.VMEM((N_Z, rows, rw), BF16),
            pltpu.VMEM((N_Z, N_EP, cap, rw), BF16),
            pltpu.VMEM((8 * N_EP, cap, hw), BF16),
            dma((6,)),
            dma, dma((N_EP,)), dma, dma((N_EP,)),
            dma, dma((N_Z, N_EP)), dma, dma((N_Z,)), dma, dma,
            dma, dma((N_Z,)),
            dma, dma, dma, dma((8,)), dma, dma,
        ],
        compiler_params=pltpu.CompilerParams(
            collective_id=0, has_side_effects=True, vmem_limit_bytes=60 * 1024 * 1024
        ),
        name="expert_layer",
    )(expert_ids, tokens, router, gate_weight, up_weight, down_weight, keep_mask)


def solution(mesh):
    return jax.shard_map(
        shards,
        mesh=mesh,
        in_specs=(
            P("ep", None),
            P("ep", None),
            P(),
            P("ep", None, "tp"),
            P("ep", None, "tp"),
            P("ep", "tp", None),
            P("ep", None),
        ),
        out_specs=P("ep", None),
        check_vma=False,
    )
```

```python
import functools

import jax
import jax.numpy as jnp
from jax import lax
from jax.experimental import pallas as pl
from jax.experimental.pallas import tpu as pltpu
from jax.sharding import PartitionSpec as P

MESH = pl.DeviceIdType.MESH
BF16 = jnp.bfloat16
F32 = jnp.float32
N_EP, N_TP = 8, 16
N_Z = 4
GW = 512
Z_HOPS = [2, 1, 3]
GROUPS = [[(0, 0), (1, 0), (0, 2), (1, 2)], [(0, 1), (0, 3), (1, 1), (1, 3)]]


def dot(a, b):
    return jnp.dot(a, b, preferred_element_type=F32)


def kernel(cap, ids_ref, tok_h, rt_h, wg_h, wu_h, wd_h, mk_h, out_ref,
           tok, rt, wg, wu, wd, mk, og, oq, xg, xq, gate, up, hid, sd, rd, tt, cb,
           lsem, g_s, g_r, q_s, q_r, z_s, z_r, dg_s, dg_r, dq_s, dq_r, rd_s, rd_r,
           m_s, m_r, a_s, a_r, da_s, da_r):
    ep = lax.axis_index("ep")
    tp = lax.axis_index("tp")
    xl, y = ep // 4, ep % 4
    xh, z, c = tp // 8, (tp // 2) % N_Z, tp % 2
    tok_rows, width = tok.shape
    qw = oq.shape[2]
    rows = N_EP * cap
    rw = width // 8
    hw = rw // 2

    def ep_at(a, b):
        return ((xl + a) % 2) * 4 + (y + b) % 4

    def tp_at(h, s, k):
        return ((xh + h) % 2) * 8 + ((z + s) % N_Z) * 2 + (c + k) % 2

    twin = tp_at(0, 0, 1)

    def remote(src, dst, ss, rs, e, t):
        return pltpu.make_async_remote_copy(src_ref=src, dst_ref=dst, send_sem=ss, recv_sem=rs, device_id=(e, t), device_id_type=MESH)

    def arrived(dst, rs):
        remote(dst, dst, rs, rs, ep, twin).wait_recv()

    def sent(src, ss):
        remote(src, src, ss, ss, ep, twin).wait_send()

    barrier = pltpu.get_barrier_semaphore()
    for a in range(2):
        for b in range(4):
            for h in range(2):
                for s in range(N_Z):
                    if a or b or h or s:
                        pl.semaphore_signal(barrier, inc=1, device_id=(ep_at(a, b), tp_at(h, s, 0)), device_id_type=MESH)
    pl.semaphore_signal(barrier, inc=1, device_id=(ep, twin), device_id_type=MESH)

    out_col = pl.multiple_of((z * 2 + c) * rw + xh * hw, 128)
    loads = [
        pltpu.make_async_copy(tok_h, tok, lsem.at[0]),
        pltpu.make_async_copy(wg_h.at[0], wg, lsem.at[1]),
        pltpu.make_async_copy(wu_h.at[0], wu, lsem.at[2]),
        pltpu.make_async_copy(wd_h.at[0], wd, lsem.at[3]),
        pltpu.make_async_copy(rt_h, rt, lsem.at[4]),
        pltpu.make_async_copy(mk_h.at[:, pl.ds(out_col, hw)], mk, lsem.at[5]),
    ]
    loads[0].start()

    with jax.named_scope("route"):
        ids = ids_ref[...].astype(F32)
        id0, id1 = ids[0:1, :], ids[1:2, :]
        esub = lax.broadcasted_iota(jnp.int32, (16, tok_rows), 0).astype(F32)
        oh0 = (esub == id0).astype(F32)
        oh1 = (esub == id1).astype(F32)
        rlane = lax.broadcasted_iota(jnp.int32, (tok_rows, tok_rows), 1)
        rsub = lax.broadcasted_iota(jnp.int32, (tok_rows, tok_rows), 0)
        before = (rsub < rlane).astype(BF16)
        count = dot((oh0 + oh1).astype(BF16), before)
        row0 = id0 * cap + jnp.sum(count * oh0, axis=0, keepdims=True)
        row1 = id1 * cap + jnp.sum(count * oh1, axis=0, keepdims=True)
        line = lax.broadcasted_iota(jnp.int32, (rows, tok_rows), 0).astype(F32)
        picker = ((line == row0) | (line == row1)).astype(BF16)
        loads[0].wait()
        for cp in loads[1:]:
            cp.start()
    with jax.named_scope("pick"):
        g_col = pl.multiple_of((z * 2 + c) * GW, 128)
        q_col = pl.multiple_of(8 * GW + c * qw, 128)
        og[...] = dot(picker, tok[:, pl.ds(g_col, GW)]).astype(BF16).reshape(N_EP, cap, GW)
        oq[...] = dot(picker, tok[:, pl.ds(q_col, qw)]).astype(BF16).reshape(N_EP, cap, qw)
        my_g = pl.ds(pl.multiple_of(c * GW, 128), GW)
        my_q = pl.ds(pl.multiple_of(c * qw, 128), qw)
        xg[z, ep, :, my_g] = og[ep]
        xq[ep, :, my_q] = oq[ep]
    with jax.named_scope("barrier"):
        pl.semaphore_wait(barrier, 64)

    for group in GROUPS:
        for a, b in group:
            if a or b:
                e = ep_at(a, b)
                remote(og.at[e], xg.at[z, ep, :, my_g], g_s, g_r.at[ep], e, tp).start()
        for a, b in group:
            if a or b:
                e = ep_at(a, b)
                remote(oq.at[e], xq.at[ep, :, my_q], q_s, q_r.at[ep], e, tp).start()

    def from_at(a, b):
        return ep_at(a, 4 - b)

    def spread(gi):
        for a, b in GROUPS[gi]:
            d = from_at(a, b)
            mine = xg.at[z, d, :, my_g]
            if a or b:
                arrived(mine, g_r.at[d])
            for s in Z_HOPS:
                remote(mine, mine, z_s, z_r.at[z, d], ep, tp_at(0, s, 0)).start()
            remote(mine, mine, dg_s, dg_r.at[gi, z], ep, twin).start()
            if not (a or b):
                remote(xq.at[d, :, my_q], xq.at[d, :, my_q], dq_s, dq_r.at[gi], ep, twin).start()

    def relay(gi):
        for a, b in GROUPS[gi]:
            d = from_at(a, b)
            for s in Z_HOPS[::-1]:
                zz = (z + s) % N_Z
                part = xg.at[zz, d, :, my_g]
                arrived(part, z_r.at[zz, d])
                remote(part, part, dg_s, dg_r.at[gi, zz], ep, twin).start()
        for a, b in GROUPS[gi]:
            d = from_at(a, b)
            if a or b:
                part = xq.at[d, :, my_q]
                arrived(part, q_r.at[d])
                remote(part, part, dq_s, dq_r.at[gi], ep, twin).start()

    def gather(ref, gi):
        return jnp.concatenate([ref[from_at(a, b)] for a, b in GROUPS[gi]], axis=0)

    def mlp(gi):
        n = len(GROUPS[gi])
        gate[...] = jnp.zeros_like(gate)
        up[...] = jnp.zeros_like(up)
        for s in [0] + Z_HOPS[::-1]:
            zz = (z + s) % N_Z
            arrived(xg.at[zz, pl.ds(0, n), :, my_g], dg_r.at[gi, zz])
            x = gather(xg.at[zz], gi)
            k = pl.ds(pl.multiple_of(zz * 2 * GW, 128), 2 * GW)
            gate[...] += dot(x, wg[k, :])
            up[...] += dot(x, wu[k, :])
        arrived(xq.at[pl.ds(0, n), :, my_q], dq_r.at[gi])
        x = gather(xq, gi)
        k = pl.ds(8 * GW, 2 * qw)
        total_gate = gate[...] + dot(x, wg[k, :])
        total_up = up[...] + dot(x, wu[k, :])
        hid[gi] = (jax.nn.silu(total_gate) * total_up).astype(BF16)

    z_order = Z_HOPS + [0]

    def down(gi):
        def down_twin(i):
            zz = (z + z_order[i]) % N_Z
            col = pl.multiple_of((zz * 2 + 1 - c) * rw, 128)
            sd[gi, i] = dot(hid[gi], wd[:, pl.ds(col, rw)]).astype(BF16)
            remote(sd.at[gi, i], rd.at[gi, i], rd_s, rd_r.at[gi, i], ep, twin).start()

        def down_own(i):
            zz = (z + z_order[i]) % N_Z
            col = pl.multiple_of((zz * 2 + c) * rw, 128)
            total = dot(hid[gi], wd[:, pl.ds(col, rw)])
            arrived(rd.at[gi, i], rd_r.at[gi, i])
            total = total + rd[gi, i].astype(F32)
            tt[gi, i] = total.astype(BF16).reshape(len(GROUPS[gi]), cap, rw)

        down_twin(0)
        down_twin(1)
        down_own(0)
        down_twin(2)
        down_own(1)
        down_twin(3)
        down_own(2)
        down_own(3)

    def scatter(gi):
        here = (xh * N_Z + z) * N_EP + ep
        n = len(GROUPS[gi])
        for t in range(4):
            for u in range(2):
                for v in range(4):
                    h = (v + u) % 2
                    i = (v + t) % 4
                    j = (v // 2 + t + u) % 2 * 2 + (v % 2) if n == 4 else 0
                    a, b = GROUPS[gi][j]
                    s = z_order[i]
                    d = from_at(a, b)
                    hcol = pl.multiple_of(((xh + h) % 2) * hw, 128)
                    if h or s or a or b:
                        remote(tt.at[gi, i, j, :, pl.ds(hcol, hw)], cb.at[here], m_s, m_r, d, tp_at(h, s, 0)).start()
                    else:
                        cb[here] = tt[gi, i, j, :, pl.ds(hcol, hw)]

    with jax.named_scope("spread0"):
        spread(0)
    with jax.named_scope("spread1"):
        spread(1)
    loads[1].wait()
    loads[2].wait()
    loads[3].wait()
    for gi in range(2):
        with jax.named_scope(f"relay{gi}"):
            relay(gi)
        with jax.named_scope(f"mlp{gi}"):
            mlp(gi)
        with jax.named_scope(f"down{gi}"):
            down(gi)
            scatter(gi)

    with jax.named_scope("gates"):
        loads[4].wait()
        loads[5].wait()
        logits = lax.dot_general(tok[...], rt[...], (((1,), (1,)), ((), ())), preferred_element_type=F32)
        eye = rlane == rsub

        def column(row):
            return jnp.sum(jnp.where(eye, row, 0.0), axis=1, keepdims=True)

        place0, place1 = column(row0), column(row1)
        elane = lax.broadcasted_iota(jnp.int32, logits.shape, 1).astype(F32)
        pick0 = jnp.sum(jnp.where(elane == column(id0), logits, 0.0), axis=1, keepdims=True)
        pick1 = jnp.sum(jnp.where(elane == column(id1), logits, 0.0), axis=1, keepdims=True)
        w0 = jax.nn.sigmoid(pick0 - pick1)
        w1 = jax.nn.sigmoid(pick1 - pick0)
        keep = mk[...].astype(F32) * 1.25
        cline = lax.broadcasted_iota(jnp.int32, (tok_rows, rows), 1).astype(F32)
        sel = jnp.concatenate([(cline == place0).astype(BF16), (cline == place1).astype(BF16)], axis=0)

    n_src = cb.shape[0]
    with jax.named_scope("m_wait"):
        arrived(cb.at[pl.ds(0, n_src - 1)], m_r)
    with jax.named_scope("combine"):
        total = cb[0:N_EP].astype(F32)
        for j in range(1, n_src // N_EP):
            total += cb[j * N_EP:(j + 1) * N_EP].astype(F32)
        both = dot(sel, total.astype(BF16).reshape(rows, hw))
        combined = w0 * both[:tok_rows] + w1 * both[tok_rows:]
        mine = pl.ds(out_col, hw)
        out_ref[:, mine] = (combined * keep).astype(BF16)

    with jax.named_scope("ag"):
        for h in (1, 0):
            for s in Z_HOPS + [0]:
                if h or s:
                    remote(out_ref.at[:, mine], out_ref.at[:, mine], a_s, a_r.at[xh * N_Z + z], ep, tp_at(h, s, 0)).start()
        remote(out_ref.at[:, mine], out_ref.at[:, mine], da_s, da_r, ep, twin).start()
        for h in (0, 1):
            for s in (0, 1, 3, 2):
                if h or s:
                    hh, zz = (xh + h) % 2, (z + s) % N_Z
                    theirs = pl.ds(pl.multiple_of((zz * 2 + c) * rw + hh * hw, 128), hw)
                    arrived(out_ref.at[:, theirs], a_r.at[hh * N_Z + zz])
                    remote(out_ref.at[:, theirs], out_ref.at[:, theirs], da_s, da_r, ep, twin).start()
        arrived(out_ref.at[:, pl.ds(0, 8 * hw)], da_r)

    sent(og.at[pl.ds(0, 7)], g_s)
    sent(oq.at[pl.ds(0, 7)], q_s)
    sent(xg.at[pl.ds(0, 3), :, :, my_g], z_s)
    sent(xg.at[:, :, :, my_g], dg_s)
    sent(oq, dq_s)
    sent(sd, rd_s)
    sent(cb.at[pl.ds(0, n_src - 1)], m_s)
    sent(out_ref.at[:, pl.ds(0, 7 * hw)], a_s)
    sent(out_ref.at[:, pl.ds(0, 8 * hw)], da_s)


def shards(tokens, expert_ids, router, gate_weight, up_weight, down_weight, keep_mask):
    tok_rows, width = tokens.shape
    hidden = gate_weight.shape[2]
    cap = 3 * tok_rows // N_EP
    rows = N_EP * cap
    qw = (width - 8 * GW) // 2
    rw = width // 8
    hw = rw // 2
    n_g = len(GROUPS)
    rows_g = rows // n_g
    any_spec = pl.BlockSpec(memory_space=pl.ANY)
    vmem_spec = pl.BlockSpec(memory_space=pltpu.VMEM)
    dma = pltpu.SemaphoreType.DMA
    return pl.pallas_call(
        functools.partial(kernel, cap),
        out_shape=jax.ShapeDtypeStruct((tok_rows, width), BF16),
        in_specs=[vmem_spec] + [any_spec] * 6,
        out_specs=vmem_spec,
        scratch_shapes=[
            pltpu.VMEM((tok_rows, width), BF16),
            pltpu.VMEM(router.shape[::-1], BF16),
            pltpu.VMEM((width, hidden), BF16),
            pltpu.VMEM((width, hidden), BF16),
            pltpu.VMEM((hidden, width), BF16),
            pltpu.VMEM((tok_rows, hw), jnp.int32),
            pltpu.VMEM((N_EP, cap, GW), BF16),
            pltpu.VMEM((N_EP, cap, qw), BF16),
            pltpu.VMEM((N_Z, N_EP, cap, 2 * GW), BF16),
            pltpu.VMEM((N_EP, cap, 2 * qw), BF16),
            pltpu.VMEM((rows_g, hidden), F32),
            pltpu.VMEM((rows_g, hidden), F32),
            pltpu.VMEM((n_g, rows_g, hidden), BF16),
            pltpu.VMEM((n_g, N_Z, rows_g, rw), BF16),
            pltpu.VMEM((n_g, N_Z, rows_g, rw), BF16),
            pltpu.VMEM((n_g, N_Z, N_EP // n_g, cap, rw), BF16),
            pltpu.VMEM((8 * N_EP, cap, hw), BF16),
            dma((6,)),
            dma, dma((N_EP,)), dma, dma((N_EP,)),
            dma, dma((N_Z, N_EP)), dma, dma((n_g, N_Z)), dma, dma((n_g,)),
            dma, dma((n_g, N_Z)),
            dma, dma, dma, dma((8,)), dma, dma,
        ],
        compiler_params=pltpu.CompilerParams(
            collective_id=0, has_side_effects=True, vmem_limit_bytes=52 * 1024 * 1024
        ),
        name="expert_layer",
    )(expert_ids.T, tokens, router.T, gate_weight, up_weight, down_weight, keep_mask)


def solution(mesh):
    return jax.shard_map(
        shards,
        mesh=mesh,
        in_specs=(
            P("ep", None),
            P("ep", None),
            P(),
            P("ep", None, "tp"),
            P("ep", None, "tp"),
            P("ep", "tp", None),
            P("ep", None),
        ),
        out_specs=P("ep", None),
        check_vma=False,
    )
```

```python
import functools

import jax
import jax.numpy as jnp
from jax import lax
from jax.experimental import pallas as pl
from jax.experimental.pallas import tpu as pltpu
from jax.sharding import PartitionSpec as P

MESH = pl.DeviceIdType.MESH
BF16 = jnp.bfloat16
F32 = jnp.float32
N_EP, N_TP = 8, 16
N_Z = 4
GW = 512
Z_HOPS = [2, 1, 3]
NC = 512
GROUPS = [[(0, 0), (1, 0), (0, 2), (1, 2)], [(0, 1), (0, 3), (1, 1), (1, 3)]]
SENDS = ['g0', 'q0', 'g1', 'q1']
STEPS = [
    "s0", "gates0", "s1", "rz0", "rq0", "w0", "mlp0", "tw0", "ow0", "rz1", "rq1", "mlp1", "tw1", "ow1",
]


def dot(a, b):
    return jnp.dot(a, b, preferred_element_type=F32)


def kernel(cap, ids_h, tok_h, rt_h, wg_h, wu_h, wd_h, mk_h, out_ref,
           ids_ref, tok, rt, wgu, wd, mk, og, oq, xx, acc, hid, sd, rd, tt, cb, wt, sel,
           lsem, g_s, g_r, q_s, q_r, z_s, z_r, dg_s, dg_r, dq_s, dq_r, rd_s, rd_r,
           m_s, m_r, a_s, a_r, da_s, da_r):
    ep = lax.axis_index("ep")
    tp = lax.axis_index("tp")
    xl, y = ep // 4, ep % 4
    xh, z, c = tp // 8, (tp // 2) % N_Z, tp % 2
    tok_rows, width = tok.shape
    qw = oq.shape[2]
    rows = N_EP * cap
    rw = width // 8
    hw = rw // 2

    def ep_at(a, b):
        return ((xl + a) % 2) * 4 + (y + b) % 4

    def tp_at(h, s, k):
        return ((xh + h) % 2) * 8 + ((z + s) % N_Z) * 2 + (c + k) % 2

    def tp_z(zz):
        return xh * 8 + zz * 2 + c

    twin = tp_at(0, 0, 1)

    def remote(src, dst, ss, rs, e, t):
        return pltpu.make_async_remote_copy(src_ref=src, dst_ref=dst, send_sem=ss, recv_sem=rs, device_id=(e, t), device_id_type=MESH)

    def arrived(dst, rs):
        remote(dst, dst, rs, rs, ep, twin).wait_recv()

    def sent(src, ss):
        remote(src, src, ss, ss, ep, twin).wait_send()

    first_loads = [
        pltpu.make_async_copy(ids_h, ids_ref, lsem.at[6]),
        pltpu.make_async_copy(tok_h, tok, lsem.at[0]),
    ]
    for cp in first_loads:
        cp.start()

    barrier = pltpu.get_barrier_semaphore()
    for a in range(2):
        for b in range(4):
            for h in range(2):
                for s in range(N_Z):
                    if a or b or h or s:
                        pl.semaphore_signal(barrier, inc=1, device_id=(ep_at(a, b), tp_at(h, s, 0)), device_id_type=MESH)
    pl.semaphore_signal(barrier, inc=1, device_id=(ep, twin), device_id_type=MESH)

    out_col = pl.multiple_of((c * N_Z + z) * rw + xh * hw, 128)
    loads = [
        pltpu.make_async_copy(rt_h, rt, lsem.at[4]),
        pltpu.make_async_copy(mk_h.at[:, pl.ds(out_col, hw)], mk, lsem.at[5]),
        pltpu.make_async_copy(wg_h.at[0], wgu.at[0], lsem.at[1]),
        pltpu.make_async_copy(wu_h.at[0], wgu.at[1], lsem.at[2]),
        pltpu.make_async_copy(wd_h.at[0], wd, lsem.at[3]),
    ]
    with jax.named_scope("route"):
        first_loads[0].wait()
        ids = ids_ref[...].astype(F32)
        id0, id1 = ids[0:1, :], ids[1:2, :]
        esub = lax.broadcasted_iota(jnp.int32, (16, tok_rows), 0).astype(F32)
        oh0 = (esub == id0).astype(F32)
        oh1 = (esub == id1).astype(F32)
        rlane = lax.broadcasted_iota(jnp.int32, (tok_rows, tok_rows), 1)
        rsub = lax.broadcasted_iota(jnp.int32, (tok_rows, tok_rows), 0)
        before = (rsub < rlane).astype(BF16)
        count = dot((oh0 + oh1).astype(BF16), before)
        row0 = id0 * cap + jnp.sum(count * oh0, axis=0, keepdims=True)
        row1 = id1 * cap + jnp.sum(count * oh1, axis=0, keepdims=True)
        line = lax.broadcasted_iota(jnp.int32, (rows, tok_rows), 0).astype(F32)
        picker = ((line == row0) | (line == row1)).astype(BF16)
        first_loads[1].wait()
        for cp in loads:
            cp.start()
    with jax.named_scope("pick"):
        g_col = pl.multiple_of((z * 2 + c) * GW, 128)
        q_col = pl.multiple_of(8 * GW + c * qw, 128)
        og[...] = dot(picker, tok[:, pl.ds(g_col, GW)]).astype(BF16).reshape(N_EP, cap, GW)
        oq[...] = dot(picker, tok[:, pl.ds(q_col, qw)]).astype(BF16).reshape(N_EP, cap, qw)
        my_g = pl.ds(g_col, GW)
        my_q = pl.ds(q_col, qw)
        xx[ep, :, my_g] = og[ep]
        xx[ep, :, my_q] = oq[ep]
    with jax.named_scope("barrier"):
        pl.semaphore_wait(barrier, 64)

    def from_at(a, b):
        return ep_at(a, 4 - b)

    def spread_block(gi, d):
        mine = xx.at[d, :, my_g]
        for s in Z_HOPS:
            remote(mine, mine, z_s, z_r.at[z, d], ep, tp_at(0, s, 0)).start()
        remote(mine, mine, dg_s, dg_r.at[gi, z], ep, twin).start()

    def spread(gi):
        for a, b in GROUPS[gi]:
            if a or b:
                d = from_at(a, b)
                arrived(xx.at[d, :, my_g], g_r.at[d])
                spread_block(gi, d)

    spread_block(0, ep)
    for item in SENDS:
        for a, b in GROUPS[int(item[1])]:
            if a or b:
                e = ep_at(a, b)
                if item[0] == "g":
                    remote(og.at[e], xx.at[ep, :, my_g], g_s, g_r.at[ep], e, tp).start()
                else:
                    remote(oq.at[e], xx.at[ep, :, my_q], q_s, q_r.at[ep], e, tp).start()
    remote(xx.at[ep, :, my_q], xx.at[ep, :, my_q], dq_s, dq_r.at[0], ep, twin).start()

    def relay_z(gi):
        for a, b in GROUPS[gi]:
            d = from_at(a, b)
            for s in Z_HOPS[::-1]:
                zz = (z + s) % N_Z
                part = xx.at[d, :, pl.ds(pl.multiple_of((zz * 2 + c) * GW, 128), GW)]
                arrived(part, z_r.at[zz, d])
                remote(part, part, dg_s, dg_r.at[gi, zz], ep, twin).start()

    def relay_q(gi):
        for a, b in GROUPS[gi]:
            d = from_at(a, b)
            if a or b:
                part = xx.at[d, :, my_q]
                arrived(part, q_r.at[d])
                remote(part, part, dq_s, dq_r.at[gi], ep, twin).start()

    def mlp(gi):
        n = len(GROUPS[gi])
        for zz in range(N_Z):
            arrived(xx.at[pl.ds(0, n), :, my_g], dg_r.at[gi, zz])
        arrived(xx.at[pl.ds(0, n), :, my_q], dq_r.at[gi])
        blocks = [from_at(a, b) for a, b in GROUPS[gi]]

        def half(i, carry):
            x = jnp.concatenate([xx[d] for d in blocks], axis=0)
            acc[i, pl.ds(0, n * cap)] = dot(x, wgu[i])
            return carry

        lax.fori_loop(0, 2, half, 0)
        own_rows = pl.ds(0, n * cap)
        hid[gi, own_rows] = (jax.nn.silu(acc[0, own_rows]) * acc[1, own_rows]).astype(BF16)

    flip1, flip3 = z + 1 - 2 * (z % 2), 3 - z
    at, other = z % 2, 1 - z % 2

    def part_cols(f, q, hp):
        return pl.ds(pl.multiple_of((f * 2 + q) * rw + hp * hw, 128), hw)

    def cols(f, core, k):
        pair = (z // 2 + 1 + f) % 2
        return pl.ds(pl.multiple_of((core * 2 + pair) * 2 * rw + k * NC, 128), NC)

    def here(f, k):
        return pl.ds(pl.multiple_of(f * 2 * rw + k * NC, 128), NC)

    def down_twin(gi):
        own_rows = pl.ds(0, len(GROUPS[gi]) * cap)

        for f in range(2):
            def to_twin(k, carry):
                sd[gi, own_rows, here(f, k)] = dot(hid[gi, own_rows], wd[:, cols(f, 1 - c, k)]).astype(BF16)
                return carry

            lax.fori_loop(0, 2 * rw // NC, to_twin, 0)
            half = pl.ds(f * 2 * rw, 2 * rw)
            remote(sd.at[gi, own_rows, half], rd.at[gi, own_rows, half], rd_s, rd_r.at[gi, f], ep, twin).start()

    def down_own(gi):
        n = len(GROUPS[gi])
        own_rows = pl.ds(0, n * cap)
        slot = (xh * N_Z + z) * N_EP + ep
        for f in range(2):
            arrived(rd.at[gi, own_rows, pl.ds(f * 2 * rw, 2 * rw)], rd_r.at[gi, f])

            def own(k, carry):
                total = dot(hid[gi, own_rows], wd[:, cols(f, c, k)]) + rd[gi, own_rows, here(f, k)].astype(F32)
                tt[gi, pl.ds(0, n), :, here(f, k)] = total.astype(BF16).reshape(n, cap, NC)
                return carry

            lax.fori_loop(0, 2 * rw // NC, own, 0)
        for t in range(4):
            for j in range(n):
                for h in (1, 0):
                    r = (t + j + 2 * h) % 4
                    a, b = GROUPS[gi][j]
                    f, q, zz = [(0, at, (z + 2) % N_Z), (1, other, flip1), (0, other, flip3), (1, at, z)][r]
                    src = tt.at[gi, j, :, part_cols(f, q, (xh + h) % 2)]
                    if h or r < 3 or a or b:
                        to = ((xh + h) % 2) * 8 + zz * 2 + c
                        remote(src, cb.at[slot], m_s, m_r, from_at(a, b), to).start()
                    else:
                        cb[slot] = tt[gi, j, :, part_cols(f, q, xh)]

    def gates(_):
        loads[0].wait()
        loads[1].wait()
        logits = lax.dot_general(tok[...], rt[...], (((1,), (1,)), ((), ())), preferred_element_type=F32)
        eye = rlane == rsub

        def column(row):
            return jnp.sum(jnp.where(eye, row, 0.0), axis=1, keepdims=True)

        place0, place1 = column(row0), column(row1)
        elane = lax.broadcasted_iota(jnp.int32, logits.shape, 1).astype(F32)
        pick0 = jnp.sum(jnp.where(elane == column(id0), logits, 0.0), axis=1, keepdims=True)
        pick1 = jnp.sum(jnp.where(elane == column(id1), logits, 0.0), axis=1, keepdims=True)
        w0 = jax.nn.sigmoid(pick0 - pick1)
        w1 = jax.nn.sigmoid(pick1 - pick0)
        wt[0] = jnp.broadcast_to(w0, wt.shape[1:])
        wt[1] = jnp.broadcast_to(w1, wt.shape[1:])
        cline = lax.broadcasted_iota(jnp.int32, (tok_rows, rows), 1).astype(F32)
        sel[...] = jnp.concatenate([(cline == place0).astype(BF16), (cline == place1).astype(BF16)], axis=0)

    def weights(_):
        for cp in loads[2:]:
            cp.wait()

    work = {"gates": gates, "w": weights, "s": spread, "rz": relay_z, "rq": relay_q, "mlp": mlp, "tw": down_twin, "ow": down_own,}
    for step in STEPS:
        with jax.named_scope(step):
            work[step[:-1]](int(step[-1]))

    n_src = cb.shape[0]
    with jax.named_scope("m_wait"):
        arrived(cb.at[pl.ds(0, n_src - 1)], m_r)
    with jax.named_scope("combine"):
        total = cb[0:N_EP].astype(F32)
        for j in range(1, n_src // N_EP):
            total += cb[j * N_EP:(j + 1) * N_EP].astype(F32)
        both = dot(sel[...], total.astype(BF16).reshape(rows, hw))
        combined = wt[0, :, 0:1] * both[:tok_rows] + wt[1, :, 0:1] * both[tok_rows:]
        keep = mk[...].astype(F32) * 1.25
        mine = pl.ds(out_col, hw)
        out_ref[:, mine] = (combined * keep).astype(BF16)

    with jax.named_scope("ag"):
        def block(hh, zz):
            return out_ref.at[:, pl.ds(pl.multiple_of((c * N_Z + zz) * rw + hh * hw, 128), hw)]

        def share(hh, across):
            part = block(hh, z)
            if across:
                remote(part, part, a_s, a_r.at[hh * N_Z + z], ep, tp_at(1, 0, 0)).start()
            for s in Z_HOPS:
                remote(part, part, a_s, a_r.at[hh * N_Z + z], ep, tp_at(0, s, 0)).start()
            remote(part, part, da_s, da_r, ep, twin).start()

        def take(hh, zz):
            arrived(block(hh, zz), a_r.at[hh * N_Z + zz])

        share(xh, True)
        take(1 - xh, z)
        share(1 - xh, False)
        for hh in (xh, 1 - xh):
            for s in (1, 3, 2):
                zz = (z + s) % N_Z
                take(hh, zz)
                remote(block(hh, zz), block(hh, zz), da_s, da_r, ep, twin).start()
        arrived(out_ref.at[:, pl.ds(0, 8 * hw)], da_r)

    sent(og.at[pl.ds(0, 7)], g_s)
    sent(oq.at[pl.ds(0, 7)], q_s)
    sent(xx.at[:, :, pl.ds(0, 3 * GW)], z_s)
    sent(xx.at[:, :, pl.ds(0, 4 * GW)], dg_s)
    sent(oq, dq_s)
    for gi in range(len(GROUPS)):
        sent(sd.at[gi, pl.ds(0, len(GROUPS[gi]) * cap)], rd_s)
    sent(cb.at[pl.ds(0, n_src - 1)], m_s)
    sent(out_ref.at[:, pl.ds(0, 7 * hw)], a_s)
    sent(out_ref.at[:, pl.ds(0, 8 * hw)], da_s)


def shards(tokens, expert_ids, router, gate_weight, up_weight, down_weight, keep_mask):
    tok_rows, width = tokens.shape
    hidden = gate_weight.shape[2]
    cap = 3 * tok_rows // N_EP
    rows = N_EP * cap
    qw = (width - 8 * GW) // 2
    rw = width // 8
    hw = rw // 2
    n_g = len(GROUPS)
    n_max = max(len(group) for group in GROUPS)
    rows_g = n_max * cap
    hbm_spec = pl.BlockSpec(memory_space=pltpu.HBM)
    vmem_spec = pl.BlockSpec(memory_space=pltpu.VMEM)
    dma = pltpu.SemaphoreType.DMA
    return pl.pallas_call(
        functools.partial(kernel, cap),
        out_shape=jax.ShapeDtypeStruct((tok_rows, width), BF16),
        in_specs=[hbm_spec] * 7,
        out_specs=vmem_spec,
        scratch_shapes=[
            pltpu.VMEM((2, tok_rows), jnp.int32),
            pltpu.VMEM((tok_rows, width), BF16),
            pltpu.VMEM(router.shape[::-1], BF16),
            pltpu.VMEM((2, width, hidden), BF16),
            pltpu.VMEM((hidden, width), BF16),
            pltpu.VMEM((tok_rows, hw), jnp.int32),
            pltpu.VMEM((N_EP, cap, GW), BF16),
            pltpu.VMEM((N_EP, cap, qw), BF16),
            pltpu.VMEM((N_EP, cap, width), BF16),
            pltpu.VMEM((2, rows_g, hidden), F32),
            pltpu.VMEM((n_g, rows_g, hidden), BF16),
            pltpu.VMEM((n_g, rows_g, 4 * rw), BF16),
            pltpu.VMEM((n_g, rows_g, 4 * rw), BF16),
            pltpu.VMEM((n_g, n_max, cap, 4 * rw), BF16),
            pltpu.VMEM((8 * N_EP, cap, hw), BF16),
            pltpu.VMEM((2, tok_rows, 128), F32),
            pltpu.VMEM((2 * tok_rows, rows), BF16),
            dma((7,)),
            dma, dma((N_EP,)), dma, dma((N_EP,)),
            dma, dma((N_Z, N_EP)), dma, dma((n_g, N_Z)), dma, dma((n_g,)),
            dma, dma((n_g, 2)),
            dma, dma, dma, dma((8,)), dma, dma,
        ],
        compiler_params=pltpu.CompilerParams(
            collective_id=0, has_side_effects=True, vmem_limit_bytes=52 * 1024 * 1024
        ),
        name="expert_layer",
    )(expert_ids.T, tokens, router.T, gate_weight, up_weight, down_weight, keep_mask)


def solution(mesh):
    return jax.shard_map(
        shards,
        mesh=mesh,
        in_specs=(
            P("ep", None),
            P("ep", None),
            P(),
            P("ep", None, "tp"),
            P("ep", None, "tp"),
            P("ep", "tp", None),
            P("ep", None),
        ),
        out_specs=P("ep", None),
        check_vma=False,
    )
```

```python
import functools

import jax
import jax.numpy as jnp
from jax import lax
from jax.experimental import pallas as pl
from jax.experimental.pallas import tpu as pltpu
from jax.sharding import PartitionSpec as P

MESH = pl.DeviceIdType.MESH
BF16 = jnp.bfloat16
F32 = jnp.float32
N_EP, N_TP = 8, 16
N_Z = 4
GW = 512
Z_HOPS = [2, 1, 3]
NC = 512
GROUPS = [[(0, 0), (1, 0), (0, 2), (1, 2)], [(0, 1), (0, 3), (1, 1), (1, 3)]]
SENDS = ['g0', 'g1', 'q0', 'q1']
STEPS = [
    "s0", "gates0", "s1", "rz0", "rq0", "w0", "mlp0", "tw0", "ow0", "rz1", "rq1", "mlp1", "tw1", "ow1",
]


def dot(a, b):
    return jnp.dot(a, b, preferred_element_type=F32)


def kernel(cap, ids_h, tok_h, rt_h, wg_h, wu_h, wd_h, mk_h, out_ref,
           ids_ref, tok, rt, wgu, wd, mk, og, oq, xx, acc, hid, sd, rd, tt, cb, wt, sel,
           lsem, g_s, g_r, q_s, q_r, z_s, z_r, dg_s, dg_r, dq_s, dq_r, rd_s, rd_r,
           m_s, m_r, a_s, a_r, da_s, da_r):
    ep = lax.axis_index("ep")
    tp = lax.axis_index("tp")
    xl, y = ep // 4, ep % 4
    xh, z, c = tp // 8, (tp // 2) % N_Z, tp % 2
    tok_rows, width = tok.shape
    qw = oq.shape[2]
    rows = N_EP * cap
    rw = width // 8
    hw = rw // 2

    def ep_at(a, b):
        return ((xl + a) % 2) * 4 + (y + b) % 4

    def tp_at(h, s, k):
        return ((xh + h) % 2) * 8 + ((z + s) % N_Z) * 2 + (c + k) % 2

    def tp_z(zz):
        return xh * 8 + zz * 2 + c

    twin = tp_at(0, 0, 1)

    def remote(src, dst, ss, rs, e, t):
        return pltpu.make_async_remote_copy(src_ref=src, dst_ref=dst, send_sem=ss, recv_sem=rs, device_id=(e, t), device_id_type=MESH)

    def arrived(dst, rs):
        remote(dst, dst, rs, rs, ep, twin).wait_recv()

    def sent(src, ss):
        remote(src, src, ss, ss, ep, twin).wait_send()

    first_loads = [
        pltpu.make_async_copy(ids_h, ids_ref, lsem.at[6]),
        pltpu.make_async_copy(tok_h, tok, lsem.at[0]),
    ]
    for cp in first_loads:
        cp.start()

    barrier = pltpu.get_barrier_semaphore()
    for a in range(2):
        for b in range(4):
            for h in range(2):
                for s in range(N_Z):
                    if a or b or h or s:
                        pl.semaphore_signal(barrier, inc=1, device_id=(ep_at(a, b), tp_at(h, s, 0)), device_id_type=MESH)
    pl.semaphore_signal(barrier, inc=1, device_id=(ep, twin), device_id_type=MESH)

    out_col = pl.multiple_of((c * N_Z + z) * rw + xh * hw, 128)
    loads = [
        pltpu.make_async_copy(rt_h, rt, lsem.at[4]),
        pltpu.make_async_copy(mk_h.at[:, pl.ds(out_col, hw)], mk, lsem.at[5]),
        pltpu.make_async_copy(wg_h.at[0], wgu.at[0], lsem.at[1]),
        pltpu.make_async_copy(wu_h.at[0], wgu.at[1], lsem.at[2]),
        pltpu.make_async_copy(wd_h.at[0], wd, lsem.at[3]),
    ]
    with jax.named_scope("route"):
        first_loads[0].wait()
        ids = ids_ref[...].astype(F32)
        id0, id1 = ids[0:1, :], ids[1:2, :]
        esub = lax.broadcasted_iota(jnp.int32, (16, tok_rows), 0).astype(F32)
        oh0 = (esub == id0).astype(F32)
        oh1 = (esub == id1).astype(F32)
        rlane = lax.broadcasted_iota(jnp.int32, (tok_rows, tok_rows), 1)
        rsub = lax.broadcasted_iota(jnp.int32, (tok_rows, tok_rows), 0)
        before = (rsub < rlane).astype(BF16)
        count = dot((oh0 + oh1).astype(BF16), before)
        row0 = id0 * cap + jnp.sum(count * oh0, axis=0, keepdims=True)
        row1 = id1 * cap + jnp.sum(count * oh1, axis=0, keepdims=True)
        line = lax.broadcasted_iota(jnp.int32, (rows, tok_rows), 0).astype(F32)
        picker = ((line == row0) | (line == row1)).astype(BF16)
        first_loads[1].wait()
        for cp in loads:
            cp.start()
    with jax.named_scope("pick"):
        g_col = pl.multiple_of((z * 2 + c) * GW, 128)
        q_col = pl.multiple_of(8 * GW + c * qw, 128)
        og[...] = dot(picker, tok[:, pl.ds(g_col, GW)]).astype(BF16).reshape(N_EP, cap, GW)
        oq[...] = dot(picker, tok[:, pl.ds(q_col, qw)]).astype(BF16).reshape(N_EP, cap, qw)
        my_g = pl.ds(g_col, GW)
        my_q = pl.ds(q_col, qw)
        xx[ep, :, my_g] = og[ep]
        xx[ep, :, my_q] = oq[ep]
    with jax.named_scope("barrier"):
        pl.semaphore_wait(barrier, 64)

    def from_at(a, b):
        return ep_at(a, 4 - b)

    def spread_block(gi, d):
        mine = xx.at[d, :, my_g]
        for s in Z_HOPS:
            remote(mine, mine, z_s, z_r.at[z, d], ep, tp_at(0, s, 0)).start()
        remote(mine, mine, dg_s, dg_r.at[gi, z], ep, twin).start()

    def spread(gi):
        for a, b in GROUPS[gi]:
            if a or b:
                d = from_at(a, b)
                arrived(xx.at[d, :, my_g], g_r.at[d])
                spread_block(gi, d)

    spread_block(0, ep)
    for item in SENDS:
        for a, b in GROUPS[int(item[1])]:
            if a or b:
                e = ep_at(a, b)
                if item[0] == "g":
                    remote(og.at[e], xx.at[ep, :, my_g], g_s, g_r.at[ep], e, tp).start()
                else:
                    remote(oq.at[e], xx.at[ep, :, my_q], q_s, q_r.at[ep], e, tp).start()
    remote(xx.at[ep, :, my_q], xx.at[ep, :, my_q], dq_s, dq_r.at[0], ep, twin).start()

    def relay_z(gi):
        for a, b in GROUPS[gi]:
            d = from_at(a, b)
            for s in Z_HOPS[::-1]:
                zz = (z + s) % N_Z
                part = xx.at[d, :, pl.ds(pl.multiple_of((zz * 2 + c) * GW, 128), GW)]
                arrived(part, z_r.at[zz, d])
                remote(part, part, dg_s, dg_r.at[gi, zz], ep, twin).start()

    def relay_q(gi):
        for a, b in GROUPS[gi]:
            d = from_at(a, b)
            if a or b:
                part = xx.at[d, :, my_q]
                arrived(part, q_r.at[d])
                remote(part, part, dq_s, dq_r.at[gi], ep, twin).start()

    def mlp(gi):
        n = len(GROUPS[gi])
        for zz in range(N_Z):
            arrived(xx.at[pl.ds(0, n), :, my_g], dg_r.at[gi, zz])
        arrived(xx.at[pl.ds(0, n), :, my_q], dq_r.at[gi])
        blocks = [from_at(a, b) for a, b in GROUPS[gi]]

        def half(i, carry):
            x = jnp.concatenate([xx[d] for d in blocks], axis=0)
            acc[i, pl.ds(0, n * cap)] = dot(x, wgu[i])
            return carry

        lax.fori_loop(0, 2, half, 0)
        own_rows = pl.ds(0, n * cap)
        hid[gi, own_rows] = (jax.nn.silu(acc[0, own_rows]) * acc[1, own_rows]).astype(BF16)

    flip1, flip3 = z + 1 - 2 * (z % 2), 3 - z
    at, other = z % 2, 1 - z % 2

    def part_cols(f, q, hp):
        return pl.ds(pl.multiple_of((f * 2 + q) * rw + hp * hw, 128), hw)

    def cols(f, core, k):
        pair = (z // 2 + 1 + f) % 2
        return pl.ds(pl.multiple_of((core * 2 + pair) * 2 * rw + k * NC, 128), NC)

    def here(f, k):
        return pl.ds(pl.multiple_of(f * 2 * rw + k * NC, 128), NC)

    def down_twin(gi):
        own_rows = pl.ds(0, len(GROUPS[gi]) * cap)

        for f in range(2):
            def to_twin(k, carry):
                sd[gi, own_rows, here(f, k)] = dot(hid[gi, own_rows], wd[:, cols(f, 1 - c, k)]).astype(BF16)
                return carry

            lax.fori_loop(0, 2 * rw // NC, to_twin, 0)
            half = pl.ds(f * 2 * rw, 2 * rw)
            remote(sd.at[gi, own_rows, half], rd.at[gi, own_rows, half], rd_s, rd_r.at[gi, f], ep, twin).start()

    def down_own(gi):
        n = len(GROUPS[gi])
        own_rows = pl.ds(0, n * cap)
        slot = (xh * N_Z + z) * N_EP + ep
        for f in range(2):
            arrived(rd.at[gi, own_rows, pl.ds(f * 2 * rw, 2 * rw)], rd_r.at[gi, f])

            def own(k, carry):
                total = dot(hid[gi, own_rows], wd[:, cols(f, c, k)]) + rd[gi, own_rows, here(f, k)].astype(F32)
                tt[gi, pl.ds(0, n), :, here(f, k)] = total.astype(BF16).reshape(n, cap, NC)
                return carry

            lax.fori_loop(0, 2 * rw // NC, own, 0)
        for t in range(4):
            for j in range(n):
                for h in (1, 0):
                    r = (t + j + 2 * h) % 4
                    a, b = GROUPS[gi][j]
                    f, q, zz = [(0, at, (z + 2) % N_Z), (1, other, flip1), (0, other, flip3), (1, at, z)][r]
                    src = tt.at[gi, j, :, part_cols(f, q, (xh + h) % 2)]
                    if h or r < 3 or a or b:
                        to = ((xh + h) % 2) * 8 + zz * 2 + c
                        remote(src, cb.at[slot], m_s, m_r, from_at(a, b), to).start()
                    else:
                        cb[slot] = tt[gi, j, :, part_cols(f, q, xh)]

    def gates(_):
        loads[0].wait()
        loads[1].wait()
        logits = lax.dot_general(tok[...], rt[...], (((1,), (1,)), ((), ())), preferred_element_type=F32)
        eye = rlane == rsub

        def column(row):
            return jnp.sum(jnp.where(eye, row, 0.0), axis=1, keepdims=True)

        place0, place1 = column(row0), column(row1)
        elane = lax.broadcasted_iota(jnp.int32, logits.shape, 1).astype(F32)
        pick0 = jnp.sum(jnp.where(elane == column(id0), logits, 0.0), axis=1, keepdims=True)
        pick1 = jnp.sum(jnp.where(elane == column(id1), logits, 0.0), axis=1, keepdims=True)
        w0 = jax.nn.sigmoid(pick0 - pick1)
        w1 = jax.nn.sigmoid(pick1 - pick0)
        wt[0] = jnp.broadcast_to(w0, wt.shape[1:])
        wt[1] = jnp.broadcast_to(w1, wt.shape[1:])
        cline = lax.broadcasted_iota(jnp.int32, (tok_rows, rows), 1).astype(F32)
        sel[...] = jnp.concatenate([(cline == place0).astype(BF16), (cline == place1).astype(BF16)], axis=0)

    def weights(_):
        for cp in loads[2:]:
            cp.wait()

    work = {"gates": gates, "w": weights, "s": spread, "rz": relay_z, "rq": relay_q, "mlp": mlp, "tw": down_twin, "ow": down_own,}
    for step in STEPS:
        with jax.named_scope(step):
            work[step[:-1]](int(step[-1]))

    n_src = cb.shape[0]
    with jax.named_scope("m_wait"):
        arrived(cb.at[pl.ds(0, n_src - 1)], m_r)
    with jax.named_scope("combine"):
        total = cb[0:N_EP].astype(F32)
        for j in range(1, n_src // N_EP):
            total += cb[j * N_EP:(j + 1) * N_EP].astype(F32)
        both = dot(sel[...], total.astype(BF16).reshape(rows, hw))
        combined = wt[0, :, 0:1] * both[:tok_rows] + wt[1, :, 0:1] * both[tok_rows:]
        keep = mk[...].astype(F32) * 1.25
        mine = pl.ds(out_col, hw)
        out_ref[:, mine] = (combined * keep).astype(BF16)

    with jax.named_scope("ag"):
        def block(hh, zz):
            return out_ref.at[:, pl.ds(pl.multiple_of((c * N_Z + zz) * rw + hh * hw, 128), hw)]

        def share(hh, across):
            part = block(hh, z)
            if across:
                remote(part, part, a_s, a_r.at[hh * N_Z + z], ep, tp_at(1, 0, 0)).start()
            for s in Z_HOPS:
                remote(part, part, a_s, a_r.at[hh * N_Z + z], ep, tp_at(0, s, 0)).start()
            remote(part, part, da_s, da_r, ep, twin).start()

        def take(hh, zz):
            arrived(block(hh, zz), a_r.at[hh * N_Z + zz])

        share(xh, True)
        take(1 - xh, z)
        share(1 - xh, False)
        for hh in (xh, 1 - xh):
            for s in (1, 3, 2):
                zz = (z + s) % N_Z
                take(hh, zz)
                remote(block(hh, zz), block(hh, zz), da_s, da_r, ep, twin).start()
        arrived(out_ref.at[:, pl.ds(0, 8 * hw)], da_r)

    sent(og.at[pl.ds(0, 7)], g_s)
    sent(oq.at[pl.ds(0, 7)], q_s)
    sent(xx.at[:, :, pl.ds(0, 3 * GW)], z_s)
    sent(xx.at[:, :, pl.ds(0, 4 * GW)], dg_s)
    sent(oq, dq_s)
    for gi in range(len(GROUPS)):
        sent(sd.at[gi, pl.ds(0, len(GROUPS[gi]) * cap)], rd_s)
    sent(cb.at[pl.ds(0, n_src - 1)], m_s)
    sent(out_ref.at[:, pl.ds(0, 7 * hw)], a_s)
    sent(out_ref.at[:, pl.ds(0, 8 * hw)], da_s)


def shards(tokens, expert_ids, router, gate_weight, up_weight, down_weight, keep_mask):
    tok_rows, width = tokens.shape
    hidden = gate_weight.shape[2]
    cap = 3 * tok_rows // N_EP
    rows = N_EP * cap
    qw = (width - 8 * GW) // 2
    rw = width // 8
    hw = rw // 2
    n_g = len(GROUPS)
    n_max = max(len(group) for group in GROUPS)
    rows_g = n_max * cap
    hbm_spec = pl.BlockSpec(memory_space=pltpu.HBM)
    vmem_spec = pl.BlockSpec(memory_space=pltpu.VMEM)
    dma = pltpu.SemaphoreType.DMA
    return pl.pallas_call(
        functools.partial(kernel, cap),
        out_shape=jax.ShapeDtypeStruct((tok_rows, width), BF16),
        in_specs=[hbm_spec] * 7,
        out_specs=vmem_spec,
        scratch_shapes=[
            pltpu.VMEM((2, tok_rows), jnp.int32),
            pltpu.VMEM((tok_rows, width), BF16),
            pltpu.VMEM(router.shape[::-1], BF16),
            pltpu.VMEM((2, width, hidden), BF16),
            pltpu.VMEM((hidden, width), BF16),
            pltpu.VMEM((tok_rows, hw), jnp.int32),
            pltpu.VMEM((N_EP, cap, GW), BF16),
            pltpu.VMEM((N_EP, cap, qw), BF16),
            pltpu.VMEM((N_EP, cap, width), BF16),
            pltpu.VMEM((2, rows_g, hidden), F32),
            pltpu.VMEM((n_g, rows_g, hidden), BF16),
            pltpu.VMEM((n_g, rows_g, 4 * rw), BF16),
            pltpu.VMEM((n_g, rows_g, 4 * rw), BF16),
            pltpu.VMEM((n_g, n_max, cap, 4 * rw), BF16),
            pltpu.VMEM((8 * N_EP, cap, hw), BF16),
            pltpu.VMEM((2, tok_rows, 128), F32),
            pltpu.VMEM((2 * tok_rows, rows), BF16),
            dma((7,)),
            dma, dma((N_EP,)), dma, dma((N_EP,)),
            dma, dma((N_Z, N_EP)), dma, dma((n_g, N_Z)), dma, dma((n_g,)),
            dma, dma((n_g, 2)),
            dma, dma, dma, dma((8,)), dma, dma,
        ],
        compiler_params=pltpu.CompilerParams(
            collective_id=0, has_side_effects=True, vmem_limit_bytes=52 * 1024 * 1024
        ),
        name="expert_layer",
    )(expert_ids.T, tokens, router.T, gate_weight, up_weight, down_weight, keep_mask)


def solution(mesh):
    return jax.shard_map(
        shards,
        mesh=mesh,
        in_specs=(
            P("ep", None),
            P("ep", None),
            P(),
            P("ep", None, "tp"),
            P("ep", None, "tp"),
            P("ep", "tp", None),
            P("ep", None),
        ),
        out_specs=P("ep", None),
        check_vma=False,
    )
```
